64 devices in a mesh: replica: 4 (over x, y), ep: 16 (over z, core).
Axes of the slice: x: 2, y: 2, z: 8, core: 2. Of those that a mesh axis runs over, the one named last changes fastest.
The devices are a block of a 4x4x8 slice.
Arguments:
- x: bfloat16 [64, 256, 2048], P(('replica', 'ep')), parts along dimension 0
- wq: bfloat16 [2048, 4096], P('ep')
- wk: bfloat16 [2048, 4096], P('ep')
- wv: bfloat16 [2048, 4096], P('ep')
- wo: bfloat16 [4096, 2048], P('ep')
- wr: float32 [2048, 128], replicated
- w1: bfloat16 [128, 2048, 768], P('ep')
- w3: bfloat16 [128, 2048, 768], P('ep')
- w2: bfloat16 [128, 768, 2048], P('ep')
- idx: int32 [64, 256, 8], P(('replica', 'ep')), parts along dimension 0
Outputs:
- output: bfloat16 [64, 256, 2048], P(('replica', 'ep')), parts along dimension 0
There are 4 independent parts. The reference program is written for one: setup_inputs(seed, part) draws one part's arguments, and reference() takes and returns one part's arrays. A program takes and returns all parts, laid end to end along the dimension named above; an argument that names none is the same for every part.
All inputs are finite; a program needn't handle non-finite values.
Results may differ from the reference program's by a relative error of at most 0.0119529.
Values are sent between devices in bfloat16 or wider.
A program may use at most 768 MiB of HBM per device.

```python
import math
import jax
import jax.numpy as jnp
from jax import lax

D = 2048
HEADS = 32
HEAD = 128
EXPERTS = 128
TOP = 8
FF = 768
SEQ = 256
NSEQ = 16
BLOCK = 128

T = NSEQ * SEQ
NHOT = max(1, TOP // 4)
EPS = 1e-6
THETA = 10000.0


def setup_inputs(seed: int = 0, part: int = 0) -> dict:
    key = jax.random.PRNGKey(seed)
    ks = jax.random.split(key, 9)
    kp = jax.random.fold_in(ks[8], part)
    kx, _, _ = jax.random.split(kp, 3)
    kh, kg = jax.random.split(jax.random.fold_in(kp, 7), 2)
    hd = HEADS * HEAD

    def w(k, shape, scale):
        return (jax.random.normal(k, shape, jnp.float32) * scale).astype(jnp.bfloat16)

    x = jax.random.normal(kx, (NSEQ, SEQ, D), jnp.float32).astype(jnp.bfloat16)
    wq = w(ks[0], (D, hd), 1.6 / math.sqrt(D))
    wk = w(ks[1], (D, hd), 1.6 / math.sqrt(D))
    wv = w(ks[2], (D, hd), 1.0 / math.sqrt(D))
    wo = w(ks[3], (hd, D), 1.5 / math.sqrt(hd))
    wr = jax.random.normal(ks[4], (D, EXPERTS), jnp.float32) / math.sqrt(D)
    w1 = w(ks[5], (EXPERTS, D, FF), 1.0 / math.sqrt(D))
    w3 = w(ks[6], (EXPERTS, D, FF), 1.0 / math.sqrt(D))
    w2 = w(ks[7], (EXPERTS, FF, D), 2.0 / math.sqrt(FF))
    nhot = max(1, TOP // 2)
    start = jax.random.randint(kh, (), 0, EXPERTS)
    hot = (start + jnp.arange(nhot)) % EXPERTS
    t = jnp.arange(T)
    int_noise = (jax.random.bits(kg, (T, EXPERTS), jnp.uint32) >> 12).astype(jnp.int32)
    hot_bonus = jnp.zeros((EXPERTS,), jnp.int32).at[hot].set((9 << 20) // 10)
    int_score = (int_noise + hot_bonus).at[t, t % EXPERTS].set(1 << 24)
    int_score = int_score * EXPERTS + jnp.arange(EXPERTS, dtype=jnp.int32)
    idx = lax.top_k(int_score, TOP)[1].astype(jnp.int32).reshape(NSEQ, SEQ, TOP)
    return dict(x=x, wq=wq, wk=wk, wv=wv, wo=wo, wr=wr, w1=w1, w3=w3, w2=w2, idx=idx)


def rmsnorm(v):
    v = v.astype(jnp.float32)
    return v * lax.rsqrt(jnp.mean(v * v, axis=-1, keepdims=True) + EPS)


def rope(z):
    n = z.shape[-3]
    half = HEAD // 2
    freq = THETA ** (-jnp.arange(half, dtype=jnp.float32) / half)
    ang = jnp.arange(n, dtype=jnp.float32)[:, None] * freq
    c = jnp.cos(ang)[:, None, :]
    s = jnp.sin(ang)[:, None, :]
    z1, z2 = z[..., :half], z[..., half:]
    return jnp.concatenate([z1 * c - z2 * s, z2 * c + z1 * s], axis=-1)


def block_plan(eid, ne, cap):
    m = eid.shape[0]
    nb = (cap + ne * (BLOCK - 1)) // BLOCK + 1
    counts = jnp.bincount(eid, length=ne + 1)[:ne]
    nblk = (counts + BLOCK - 1) // BLOCK
    bend = jnp.cumsum(nblk)
    first = jnp.cumsum(counts) - counts
    order = jnp.argsort(eid)
    se = eid[order]
    sc = jnp.minimum(se, ne - 1)
    slot = jnp.where(se < ne, (bend[sc] - nblk[sc]) * BLOCK + jnp.arange(m) - first[sc], nb * BLOCK)
    cand = jnp.full((nb * BLOCK,), m, jnp.int32).at[slot].set(order.astype(jnp.int32), mode='drop')
    blk_e = jnp.minimum(jnp.searchsorted(bend, jnp.arange(nb), side='right'), ne - 1)
    return cand.reshape(nb, BLOCK), blk_e, bend[-1]


def expert_sum(rows, eid, gates, k, w1, w3, w2, cap):
    n, d = rows.shape
    ne = w1.shape[0]
    m = n * k
    cand, blk_e, nused = block_plan(eid, ne, cap)
    ok = cand < m
    row = jnp.where(ok, cand // k, 0)
    gate = jnp.where(ok, gates[jnp.minimum(cand, m - 1)], 0.0)

    def body(acc, xs):
        b, rb, gb, e = xs

        def work(acc):
            xb = rows[rb]
            a1 = jnp.dot(xb, w1[e], preferred_element_type=jnp.float32)
            a3 = jnp.dot(xb, w3[e], preferred_element_type=jnp.float32)
            act = (jax.nn.silu(a1) * a3).astype(jnp.bfloat16)
            o = jnp.dot(act, w2[e], preferred_element_type=jnp.float32).astype(jnp.bfloat16)
            return acc.at[rb].add(gb[:, None] * o.astype(jnp.float32))

        return lax.cond(b < nused, work, lambda acc: acc, acc), None

    acc, _ = lax.scan(body, jnp.zeros((n, d), jnp.float32), (jnp.arange(cand.shape[0]), row, gate, blk_e))
    return acc


def reference(x, wq, wk, wv, wo, wr, w1, w3, w2, idx):
    xf = x.reshape(T, D)
    a = rmsnorm(xf).astype(jnp.bfloat16)

    def proj(w):
        return jnp.dot(a, w, preferred_element_type=jnp.float32).reshape(NSEQ, SEQ, HEADS, HEAD)

    q = rope(proj(wq)).astype(jnp.bfloat16)
    k = rope(proj(wk)).astype(jnp.bfloat16)
    v = proj(wv).astype(jnp.bfloat16)
    causal = jnp.tril(jnp.ones((SEQ, SEQ), bool))

    def one_seq(qkv):
        qs, ks, vs = qkv
        s = jnp.einsum('qhe,khe->hqk', qs.astype(jnp.float32), ks.astype(jnp.float32)) / math.sqrt(HEAD)
        p = jax.nn.softmax(jnp.where(causal, s, -jnp.inf), axis=-1).astype(jnp.bfloat16)
        return jnp.einsum('hqk,khe->qhe', p.astype(jnp.float32), vs.astype(jnp.float32)).astype(jnp.bfloat16)

    o = lax.map(one_seq, (q, k, v))
    ao = jnp.dot(o.reshape(T, HEADS * HEAD), wo, preferred_element_type=jnp.float32)
    h = (xf.astype(jnp.float32) + ao).astype(jnp.bfloat16)
    ids = idx.reshape(T, TOP)
    r = rmsnorm(h)
    logits = jnp.dot(r, wr, precision=lax.Precision.HIGHEST, preferred_element_type=jnp.float32)
    g = jax.nn.softmax(jnp.take_along_axis(logits, ids, axis=1), axis=-1)
    moe = expert_sum(r.astype(jnp.bfloat16), ids.reshape(-1), g.reshape(-1), TOP, w1, w3, w2, T * TOP)
    return (h.astype(jnp.float32) + moe).astype(jnp.bfloat16).reshape(NSEQ, SEQ, D)
```

```python
import functools
import math
import jax
import jax.numpy as jnp
from jax import lax
from jax.experimental import pallas as pl
from jax.experimental.pallas import tpu as pltpu
from jax.sharding import PartitionSpec as P

HEAD = 128
EPS = 1e-6
THETA = 10000.0
BLK = 256
SPM = 128
DENSE_AT = 32
LANES = 128
CHUNKS = 2


def rmsnorm(v):
    v = v.astype(jnp.float32)
    return v * lax.rsqrt(jnp.mean(v * v, axis=-1, keepdims=True) + EPS)


def attention_kernel(x_hbm, idx_hbm, wq_hbm, wk_hbm, wv_hbm, wo_hbm, cos_ref, sin_ref, h_ref, idx_ref,
                     xall, wqkv, stage, wov, obuf, orecv, acc, lsem, xs_s, xs_r, ix_s, ix_r, wa_s, wa_r, wb_s, wb_r,
                     wd_s, wd_r, oz_s, oz_r, oxy_s, oxy_r, od_s, od_r, oo_s, oo_r, *, nr, ne):
    side = math.isqrt(nr)
    nz = ne // 2
    far = nz // 2
    s, d = x_hbm.shape
    wrows, cols = wqkv.shape[1] // ne, wqkv.shape[2]
    orows = wov.shape[1] // 2
    quart = s // 4
    piece = orows // 4
    r, e = lax.axis_index('replica'), lax.axis_index('ep')
    z, c = e // 2, e % 2
    px, py = r // side, r % side
    qx, qy = px % 2, py % 2
    q = 2 * qx + qy
    me = 2 * q + c
    par = (qx + qy) % 2
    rx = r + side * (1 - 2 * qx)
    ry = r + (1 - 2 * qy)
    rd = rx + (1 - 2 * qy)
    jx, jy, jd = 2 * (1 - qx) + qy, 2 * qx + (1 - qy), 2 * (1 - qx) + (1 - qy)
    ep_other = 2 * z + 1 - c
    ring = (2 * ((z + 1) % nz) + c, 2 * ((z + nz - 1) % nz) + c)

    def quad(j):
        return (px - qx + j // 2) * side + (py - qy + j % 2)

    def came(way, dist):
        return (z + nz - dist) % nz if way == 0 else (z + dist) % nz

    def remote(src, dst, ssem, rsem, rep, ep):
        return pltpu.make_async_remote_copy(src_ref=src, dst_ref=dst, send_sem=ssem, recv_sem=rsem,
                                            device_id={'replica': rep, 'ep': ep}, device_id_type=pl.DeviceIdType.MESH)

    def al(v, m):
        return pl.multiple_of(v, m)

    loads = [pltpu.make_async_copy(x_hbm, xall.at[me], lsem.at[0])]
    for w, ref in enumerate((wq_hbm, wk_hbm, wv_hbm)):
        loads.append(pltpu.make_async_copy(ref.at[:, pl.ds(al(me * cols, cols), cols)],
                                           wqkv.at[w, pl.ds(al(e * wrows, wrows), wrows)], lsem.at[1 + w]))
        loads.append(pltpu.make_async_copy(ref.at[:, pl.ds(al((2 * q + 1 - c) * cols, cols), cols)],
                                           stage.at[w, z], lsem.at[4 + w]))
    loads.append(pltpu.make_async_copy(wo_hbm, wov.at[z, pl.ds(al(c * orows, orows), orows)], lsem.at[7]))
    loads.append(pltpu.make_async_copy(idx_hbm.at[q], idx_ref.at[q], lsem.at[8]))
    for cp in loads:
        cp.start()

    barrier = pltpu.get_barrier_semaphore()
    peers = [(rx, e), (ry, e), (rd, e), (r, ep_other), (rx, ep_other), (ry, ep_other), (rd, ep_other), (r, ring[0]), (r, ring[1])]
    for rep, ep in peers:
        pl.semaphore_signal(barrier, inc=1, device_id={'replica': rep, 'ep': ep}, device_id_type=pl.DeviceIdType.MESH)
    pl.semaphore_wait(barrier, len(peers))
    for cp in loads:
        cp.wait()

    sends = []

    def go(*a):
        cp = remote(*a)
        cp.start()
        sends.append(cp)

    def part_a(zz):
        return wqkv.at[:, pl.ds(al((2 * zz + c) * wrows, wrows), wrows)]

    def part_b(zz):
        return stage.at[:, zz]

    def send_w(zz, way, dist):
        if dist <= far - way:
            go(part_a(zz), part_a(zz), wa_s.at[way, dist - 1], wa_r.at[way, dist - 1], r, ring[way])
        if dist <= far - 1 + way:
            go(part_b(zz), part_b(zz), wb_s.at[way, dist - 1], wb_r.at[way, dist - 1], r, ring[way])

    def cross_w(zz, k):
        go(part_b(zz), part_a(zz), wd_s.at[k], wd_r.at[zz], r, ep_other)

    for way in range(2):
        send_w(z, way, 1)
    for rep, k in ((rx, 0), (ry, 1), (rd, 2)):
        go(xall.at[me], xall.at[me], xs_s.at[k], xs_r.at[me], rep, e)
    cross_w(z, 0)
    go(xall.at[me], xall.at[me], xs_s.at[3], xs_r.at[me], r, ep_other)
    for k in range(4):
        @pl.when(q != k)
        def _():
            remote(idx_hbm.at[k], idx_ref.at[q], ix_s.at[k], ix_r.at[q], quad(k), e).start()

    def wait_w(dist):
        for way in range(2):
            zz = came(way, dist)
            if dist <= far - way:
                remote(part_a(zz), part_a(zz), wa_s.at[way, dist - 1], wa_r.at[way, dist - 1], r, e).wait_recv()
                if dist + 1 <= far - way:
                    go(part_a(zz), part_a(zz), wa_s.at[way, dist], wa_r.at[way, dist], r, ring[way])
            if dist <= far - 1 + way:
                remote(part_b(zz), part_b(zz), wb_s.at[way, dist - 1], wb_r.at[way, dist - 1], r, e).wait_recv()
                if dist + 1 <= far - 1 + way:
                    go(part_b(zz), part_b(zz), wb_s.at[way, dist], wb_r.at[way, dist], r, ring[way])
                cross_w(zz, 1 + 2 * (dist - 1) + way if dist < far else nz - 1)

    def pass_x(j, k):
        at = xall.at[2 * j + c]
        remote(at, at, xs_s.at[k], xs_r.at[2 * j + c], r, e).wait_recv()
        go(at, at, xs_s.at[k], xs_r.at[2 * j + c], r, ep_other)

    def half_piece(zz, h, p):
        return wov.at[zz, pl.ds(al(c * orows + 2 * piece * p + piece * h, piece), piece)]

    def send_o_ring(zz, h, way, i):
        go(half_piece(zz, h, par), half_piece(zz, h, par), oz_s.at[way, i], oz_r.at[way, i], r, ring[way])

    steps = 2 * (far - 1) + 1

    def order(way, i):
        return (1 + i // 2, i % 2) if i < steps - 1 else (far, way)

    def serve(i):
        for way in range(2):
            dist, h = order(way, i)
            zz = came(way, dist)
            at = half_piece(zz, h, par)
            remote(at, at, oz_s.at[way, i], oz_r.at[way, i], r, e).wait_recv()
            if i + 2 < steps - 1:
                send_o_ring(zz, h, way, i + 2)
            elif dist == far - 1 and h == way:
                send_o_ring(zz, h, way, steps - 1)
            go(at, at, oxy_s.at[way, i], oxy_r.at[way, i], rx if h == 0 else ry, e)
            go(at, at, od_s.at[way, i], od_r.at[zz], r, ep_other)

    def serve_side(i):
        for way in range(2):
            dist, h = order(way, i)
            zz = came(way, dist)
            at = half_piece(zz, h, 1 - par)
            remote(at, at, oxy_s.at[way, i], oxy_r.at[way, i], r, e).wait_recv()
            go(at, at, od_s.at[2 + way, i], od_r.at[zz], r, ep_other)

    for dist in range(1, far):
        wait_w(dist)
        if dist == max(1, far - 2):
            pass_x(jx, 4)
            pass_x(jy, 5)
    for h in range(2):
        for way in range(2):
            send_o_ring(z, h, way, h)
    own = wov.at[z, pl.ds(al(c * orows, orows), orows)]
    go(own, own, od_s.at[4, 0], od_r.at[z], r, ep_other)
    pass_x(jd, 6)
    wait_w(far)
    for zz in range(nz):
        at = wqkv.at[:, pl.ds((2 * zz + 1 - c) * wrows, wrows)]
        remote(at, at, wd_s.at[0], wd_r.at[zz], r, e).wait_recv()
    for j in range(4):
        at = xall.at[2 * j + 1 - c]
        remote(at, at, xs_s.at[0], xs_r.at[2 * j + 1 - c], r, e).wait_recv()

    nh = cols // HEAD
    scale = 1.0 / math.sqrt(HEAD)

    def send_o(t):
        j, cc = t // 2, t % 2
        for k in range(4):
            src = obuf.at[t, pl.ds(quart * k, quart)]
            dst = orecv.at[me, pl.ds(al(quart * j, quart), quart)]

            @pl.when((q != k) | (c != cc))
            def _():
                remote(src, dst, oo_s.at[t, k], oo_r.at[me], quad(k), 2 * z + cc).start()

            @pl.when((q == k) & (c == cc))
            def _():
                dst[...] = src[...]

    def sequence(t, _):
        xf = xall[t].astype(jnp.float32)
        a = (xf * lax.rsqrt(jnp.mean(xf * xf, axis=-1, keepdims=True) + EPS)).astype(jnp.bfloat16)
        qf = jnp.dot(a, wqkv[0], preferred_element_type=jnp.float32)
        kf = jnp.dot(a, wqkv[1], preferred_element_type=jnp.float32)
        vf = jnp.dot(a, wqkv[2], preferred_element_type=jnp.float32)
        cs, sn = cos_ref[...], sin_ref[...]
        row = lax.broadcasted_iota(jnp.int32, (s, s), 0)
        col = lax.broadcasted_iota(jnp.int32, (s, s), 1)
        for n in range(nh):
            at = slice(n * HEAD, (n + 1) * HEAD)
            qh, kh = qf[:, at], kf[:, at]
            qh = (qh * cs + pltpu.roll(qh, HEAD // 2, 1) * sn).astype(jnp.bfloat16)
            kh = (kh * cs + pltpu.roll(kh, HEAD // 2, 1) * sn).astype(jnp.bfloat16)
            sc = lax.dot_general(qh, kh, (((1,), (1,)), ((), ())), preferred_element_type=jnp.float32) * scale
            sc = jnp.where(row >= col, sc, -1e30)
            p = jnp.exp(sc - jnp.max(sc, axis=-1, keepdims=True))
            p = (p * (1.0 / jnp.sum(p, axis=-1, keepdims=True))).astype(jnp.bfloat16)
            obuf[t, :, at] = jnp.dot(p, vf[:, at].astype(jnp.bfloat16), preferred_element_type=jnp.float32).astype(jnp.bfloat16)

        @pl.when(t > 0)
        def _():
            send_o(t - 1)
        return 0

    lax.fori_loop(0, 4, sequence, 0)
    serve(0)
    lax.fori_loop(4, 8, sequence, 0)
    serve(1)
    serve_side(0)
    send_o(7)
    serve(2)
    serve_side(1)

    for k in range(8):
        @pl.when(k != me)
        def _():
            at = orecv.at[k]
            remote(at, at, oo_s.at[0, 0], oo_r.at[k], r, e).wait_recv()

    for j in range(4):
        acc[pl.ds(quart * j, quart), :] = xall[2 * j + c, pl.ds(al(quart * q, quart), quart), :].astype(jnp.float32)

    def project(zz):
        at = wov.at[zz, pl.ds(al((1 - c) * orows, orows), orows)]
        remote(at, at, od_s.at[0, 0], od_r.at[zz], r, e).wait_recv()
        width = min(512, d)

        def chunk(n, _):
            cut = pl.ds(al(n * width, width), width)
            acc[:, cut] = acc[:, cut] + jnp.dot(orecv[zz], wov[zz, :, cut], preferred_element_type=jnp.float32)
            return 0

        lax.fori_loop(0, d // width, chunk, 0)

    project(z)
    for i in range(3, steps):
        serve(i)
        serve_side(i - 1)
        if i % 2 == 1 and i // 2 < far:
            for way in range(2):
                project(came(way, i // 2))
    serve_side(steps - 1)
    for way in range(2):
        project(came(way, far - 1))
    project(came(0, far))
    h_ref[...] = acc[...].astype(jnp.bfloat16)
    for k in range(4):
        @pl.when(q != k)
        def _():
            remote(idx_hbm.at[k], idx_ref.at[k], ix_s.at[k], ix_r.at[k], r, e).wait()
    for t in range(8):
        for k in range(4):
            src = obuf.at[t, pl.ds(quart * k, quart)]

            @pl.when((q != k) | (c != t % 2))
            def _():
                remote(src, src, oo_s.at[t, k], oo_r.at[0], r, e).wait_send()
    for cp in sends:
        cp.wait_send()


def attention_call(x, idx, wq, wk, wv, wo, nr, ne):
    s, d = x.shape
    hd = wq.shape[1]
    cols = hd // 8
    nz = ne // 2
    steps = nz - 1
    half = HEAD // 2
    freq = THETA ** (-jnp.arange(half, dtype=jnp.float32) / half)
    ang = jnp.arange(s, dtype=jnp.float32)[:, None] * freq
    cos, sin = jnp.cos(ang), jnp.sin(ang)
    cos = jnp.concatenate([cos, cos], axis=1)
    sin = jnp.concatenate([-sin, sin], axis=1)
    any_ = pl.BlockSpec(memory_space=pl.ANY)
    vmem = pl.BlockSpec(memory_space=pltpu.VMEM)
    bf = jnp.bfloat16
    dma = pltpu.SemaphoreType.DMA
    return pl.pallas_call(
        functools.partial(attention_kernel, nr=nr, ne=ne),
        out_shape=(jax.ShapeDtypeStruct((s, d), bf), jax.ShapeDtypeStruct(idx.shape, idx.dtype)),
        in_specs=[any_, any_, any_, any_, any_, any_, vmem, vmem],
        out_specs=(vmem, vmem),
        scratch_shapes=[
            pltpu.VMEM((8, s, d), bf),
            pltpu.VMEM((3, d, cols), bf),
            pltpu.VMEM((3, nz, d // ne, cols), bf),
            pltpu.VMEM((nz, 2 * wo.shape[0], d), bf),
            pltpu.VMEM((8, s, cols), bf),
            pltpu.VMEM((8, s, cols), bf),
            pltpu.VMEM((s, d), jnp.float32),
            dma((9,)), dma((7,)), dma((8,)), dma((4,)), dma((4,)),
            dma((2, nz // 2)), dma((2, nz // 2)), dma((2, nz // 2)), dma((2, nz // 2)),
            dma((nz,)), dma((nz,)),
            dma((2, steps)), dma((2, steps)), dma((2, steps)), dma((2, steps)),
            dma((5, steps)), dma((nz,)), dma((8, 4)), dma((8,)),
        ],
        compiler_params=pltpu.CompilerParams(collective_id=0, has_side_effects=True, vmem_limit_bytes=60 * 2**20),
        cost_estimate=pl.CostEstimate(flops=100 * 10**9, bytes_accessed=30 * 10**6, transcendentals=10**6),
        name='attention',
    )(x, idx, wq, wk, wv, wo, cos, sin)


def router(h, wr, ids):
    r = rmsnorm(h)
    logits = jnp.dot(r, wr, precision=lax.Precision.HIGHEST, preferred_element_type=jnp.float32)
    hot = ids[:, :, None] == jnp.arange(wr.shape[1], dtype=jnp.int32)
    picked = jnp.sum(jnp.where(hot, logits[:, None, :], 0.0), axis=-1)
    return r.astype(jnp.bfloat16), jax.nn.softmax(picked, axis=-1)


def expert_kernel(nsp_ref, dense_ref, list_ref, glist_ref, gate_ref, u_hbm, w1, w3, w2, out_hbm,
                  u3, acc, ubuf, wup, wdown, act, xs, zs, sems, *, cap, run):
    ne, d, f = w1.shape
    t = u_hbm.shape[0]
    nb = t // BLK
    seg = d // LANES
    per = BLK // run
    ndev = t // (4 * run)

    def fetch(slot, e):
        pltpu.make_async_copy(w1.at[e], wup.at[slot, 0], sems.at[slot, 0]).start()
        pltpu.make_async_copy(w3.at[e], wup.at[slot, 1], sems.at[slot, 1]).start()
        pltpu.make_async_copy(w2.at[e], wdown.at[slot], sems.at[slot, 2]).start()

    def load(b):
        b = jnp.asarray(b, jnp.int32)
        j, first = b // (nb // 4), (b % (nb // 4)) * per
        for k in range(per):
            src = u_hbm.at[pl.ds(pl.multiple_of(((first + k) * 4 + j) * run, run), run)]
            pltpu.make_async_copy(src, ubuf.at[b % 2, pl.ds(k * run, run)], sems.at[2, b % 2]).start()

    load(0)
    load(1)
    fetch(0, 0)
    acc[...] = jnp.zeros_like(acc)
    u3[pl.ds(t * seg, seg), :] = jnp.zeros((seg, LANES), jnp.float32)

    def widen(b, _):
        at = ubuf.at[b % 2]
        pltpu.make_async_copy(at, at, sems.at[2, b % 2]).wait()
        for j in range(seg):
            u3[pl.ds(b * BLK * seg + j, BLK, stride=seg), :] = at[:, j * LANES:(j + 1) * LANES].astype(jnp.float32)

        @pl.when(b + 2 < nb)
        def _():
            load(b + 2)
        return 0

    lax.fori_loop(0, nb, widen, 0)
    x = ubuf.at[0]

    def hidden(slot, rows):
        for c in range(0, f, BLK):
            a1 = jnp.dot(x[:rows, :], wup[slot, 0, :, c:c + BLK], preferred_element_type=jnp.float32)
            a3 = jnp.dot(x[:rows, :], wup[slot, 1, :, c:c + BLK], preferred_element_type=jnp.float32)
            act[:rows, c:c + BLK] = (jax.nn.silu(a1) * a3).astype(jnp.bfloat16)

    def expert(e, _):
        slot = lax.rem(e, 2)

        @pl.when(e + 1 < ne)
        def _():
            fetch(1 - slot, e + 1)

        for j in range(2):
            pltpu.make_async_copy(wup.at[slot, j], wup.at[slot, j], sems.at[slot, j]).wait()
        pltpu.make_async_copy(wdown.at[slot], wdown.at[slot], sems.at[slot, 2]).wait()

        def block(b, _):
            @pl.when(dense_ref[e * nb + b] != 0)
            def _():
                r0 = pl.multiple_of(b * BLK, BLK)
                for j in range(seg):
                    x[:, j * LANES:(j + 1) * LANES] = u3[pl.ds(r0 * seg + j, BLK, stride=seg), :].astype(jnp.bfloat16)
                hidden(slot, BLK)
                lane = lax.broadcasted_iota(jnp.int32, (BLK, LANES), 1)
                g = jnp.sum(jnp.where(lane == e, gate_ref[pl.ds(r0, BLK), :], 0.0), axis=1, keepdims=True)
                for c in range(0, d, 2 * BLK):
                    z = jnp.dot(act[...], wdown[slot, :, c:c + 2 * BLK], preferred_element_type=jnp.float32)
                    z = z.astype(jnp.bfloat16).astype(jnp.float32)
                    z = jnp.where(g != 0.0, g * z, 0.0)
                    for j in range(2 * BLK // LANES):
                        at = pl.ds(r0 * seg + c // LANES + j, BLK, stride=seg)
                        acc[at, :] = acc[at, :] + z[:, j * LANES:(j + 1) * LANES]
            return 0

        lax.fori_loop(0, nb, block, 0)
        n = nsp_ref[e]

        def tile(i, _):
            base = e * cap + i * SPM
            groups = (jnp.minimum(n - i * SPM, SPM) + 7) // 8

            def gather(q, _):
                for s in range(8):
                    tok = list_ref[base + q * 8 + s]
                    xs[pl.ds(pl.multiple_of((q * 8 + s) * seg, seg), seg), :] = u3[pl.ds(pl.multiple_of(tok * seg, seg), seg), :]
                return 0

            lax.fori_loop(0, groups, gather, 0)
            for j in range(seg):
                x[:SPM, j * LANES:(j + 1) * LANES] = xs[pl.ds(j, SPM, stride=seg), :].astype(jnp.bfloat16)
            hidden(slot, SPM)
            for c in range(0, d, 2 * BLK):
                z = jnp.dot(act[:SPM, :], wdown[slot, :, c:c + 2 * BLK], preferred_element_type=jnp.float32)
                z = z.astype(jnp.bfloat16).astype(jnp.float32)
                for j in range(2 * BLK // LANES):
                    zs[pl.ds(c // LANES + j, SPM, stride=seg), :] = z[:, j * LANES:(j + 1) * LANES]

            def scatter(q, _):
                for s in range(8):
                    tok = list_ref[base + q * 8 + s]
                    g = glist_ref[base + q * 8 + s]
                    at = pl.ds(pl.multiple_of(tok * seg, seg), seg)
                    acc[at, :] = acc[at, :] + g * zs[pl.ds(pl.multiple_of((q * 8 + s) * seg, seg), seg), :]
                return 0

            lax.fori_loop(0, groups, scatter, 0)
            return 0

        lax.fori_loop(0, (n + SPM - 1) // SPM, tile, 0)
        return 0

    lax.fori_loop(0, ne, expert, 0)

    def store(k, _):
        for j in range(4):
            src = acc.at[pl.ds(pl.multiple_of((j * ndev + k) * run * seg, run * seg), run * seg)]
            dst = out_hbm.at[pl.ds(pl.multiple_of((k * 4 + j) * run * seg, run * seg), run * seg)]
            pltpu.make_async_copy(src, dst, sems.at[2, 2]).start()
        return 0

    lax.fori_loop(0, ndev, store, 0)
    pltpu.make_async_copy(acc.at[pl.ds(0, t * seg)], out_hbm, sems.at[2, 2]).wait()


def expert_call(u, gates, nsp, dense, rows, glist, w1, w3, w2, run):
    t, d = u.shape
    ne, _, f = w1.shape
    cap = rows.shape[0] // ne
    seg = d // LANES
    any_ = pl.BlockSpec(memory_space=pl.ANY)
    smem = pl.BlockSpec(memory_space=pltpu.SMEM)
    return pl.pallas_call(
        functools.partial(expert_kernel, cap=cap, run=run),
        out_shape=jax.ShapeDtypeStruct((t * seg, LANES), jnp.float32),
        in_specs=[smem] * 4 + [pl.BlockSpec(memory_space=pltpu.VMEM)] + [any_] * 4,
        out_specs=any_,
        scratch_shapes=[
            pltpu.VMEM(((t + 1) * seg, LANES), jnp.float32),
            pltpu.VMEM(((t + 1) * seg, LANES), jnp.float32),
            pltpu.VMEM((2, BLK, d), jnp.bfloat16),
            pltpu.VMEM((2, 2, d, f), jnp.bfloat16),
            pltpu.VMEM((2, f, d), jnp.bfloat16),
            pltpu.VMEM((BLK, f), jnp.bfloat16),
            pltpu.VMEM((SPM * seg, LANES), jnp.float32),
            pltpu.VMEM((SPM * seg, LANES), jnp.float32),
            pltpu.SemaphoreType.DMA((3, 3)),
        ],
        compiler_params=pltpu.CompilerParams(vmem_limit_bytes=62 * 2**20),
        cost_estimate=pl.CostEstimate(flops=60 * 10**9, bytes_accessed=160 * 10**6, transcendentals=10**6),
        name='experts',
    )(nsp, dense, rows, glist, gates, u, w1, w3, w2)


def plan(ids, g, eids):
    t = ids.shape[0]
    ne = eids.shape[0]
    nb = t // BLK
    cap = nb * DENSE_AT
    eq = ids[:, :, None] == eids
    gates = jnp.sum(jnp.where(eq, g[:, :, None], 0.0), axis=1)
    m = jnp.any(eq, axis=1)
    dense = jnp.sum(m.reshape(nb, BLK, ne), axis=1, dtype=jnp.int32) >= DENSE_AT
    sp = m & ~jnp.repeat(dense, BLK, axis=0)
    spb = sp.astype(jnp.bfloat16).reshape(t // LANES, LANES, ne)
    tri = (jnp.arange(LANES)[None, :] < jnp.arange(LANES)[:, None]).astype(jnp.bfloat16)
    inner = jnp.einsum('ij,bje->bie', tri, spb, preferred_element_type=jnp.float32)
    tot = jnp.sum(spb.astype(jnp.float32), axis=1)
    nt = t // LANES
    before = jnp.sum(jnp.where((jnp.arange(nt)[None, :] < jnp.arange(nt)[:, None])[:, :, None], tot[None], 0.0), axis=1)
    pos = (inner + before[:, None, :]).reshape(t, ne).astype(jnp.int32)
    pos = jnp.where(sp, pos, -1)
    nsp = jnp.sum(sp, axis=0, dtype=jnp.int32)
    at = pos.T[:, None, :] == jnp.arange(cap)[None, :, None]
    rows = jnp.sum(jnp.where(at, jnp.arange(t)[None, None, :] - t, 0), axis=-1, dtype=jnp.int32) + t
    glist = jnp.sum(jnp.where(at, gates.T[:, None, :], 0.0), axis=-1)
    gates = jnp.pad(gates, ((0, 0), (0, LANES - ne)))
    return gates, nsp, dense.T.reshape(-1).astype(jnp.int32), rows.reshape(-1), glist.reshape(-1)


def solution(mesh):
    nr, nd = mesh.shape['replica'], mesh.shape['ep']
    side = math.isqrt(nr)
    tok = P(('replica', 'ep'), None, None)
    rows_ep = P('ep', None)
    by_expert = P('ep', None, None)
    quads = [[(bx + j // 2) * side + by + j % 2 for j in range(4)] for bx in range(0, side, 2) for by in range(0, side, 2)]

    def local(x, wq, wk, wv, wo, wr, w1, w3, w2, idx):
        b, s, d = x.shape
        t, k, ne = b * s, idx.shape[-1], w1.shape[0]
        me = lax.axis_index('ep')
        quart = t // 4
        own = jnp.pad(idx.reshape(t, k), ((0, 0), (0, LANES - k))).reshape(4, quart, LANES)
        h, ids = attention_call(x.reshape(t, d), own, wq, wk, wv, wo, nr, nd)
        ids = ids.reshape(t, LANES)[:, :k]
        u, g = router(h, wr, ids)
        run = quart // CHUNKS
        u4, h4 = u.reshape(4, quart, d), h.reshape(4, quart, d)
        us = [lax.all_gather(u4[:, i * run:(i + 1) * run].reshape(4 * run, d), 'ep', axis=0, tiled=True) for i in range(CHUNKS)]
        gi = lax.all_gather(jnp.concatenate([g, ids.astype(jnp.float32)], axis=1), 'ep', axis=0, tiled=False)
        gi = gi.reshape(nd, 4, quart, 2 * k)
        eids = me * ne + jnp.arange(ne)
        ys = []
        for i in range(CHUNKS):
            part = gi[:, :, i * run:(i + 1) * run].transpose(1, 0, 2, 3).reshape(-1, 2 * k)
            acc = expert_call(us[i], *plan(part[:, k:].astype(jnp.int32), part[:, :k], eids), w1, w3, w2, run)
            moe = lax.psum_scatter(acc, 'ep', scatter_dimension=0, tiled=True)
            moe = moe.reshape(4, run, d)
            ys.append((h4[:, i * run:(i + 1) * run].astype(jnp.float32) + moe).astype(jnp.bfloat16))
        y = jnp.concatenate(ys, axis=1)
        y = lax.all_to_all(y, 'replica', 0, 0, axis_index_groups=quads, tiled=True)
        return y.reshape(b, s, d)

    return jax.shard_map(local, mesh=mesh,
                         in_specs=(tok, rows_ep, rows_ep, rows_ep, rows_ep, P(None, None),
                                   by_expert, by_expert, by_expert, tok),
                         out_specs=tok, check_vma=False)
```

```python
import functools
import math
import types
import jax
import jax.numpy as jnp
import numpy as np
from jax import lax
from jax.experimental import pallas as pl
from jax.experimental.pallas import tpu as pltpu
from jax.sharding import PartitionSpec as P

HEAD = 128
EPS = 1e-6
THETA = 10000.0
SPM = 128
DENSE_AT = 32
LANES = 128
FU = 2
RUNS = (32, 32)


WAYS = range(2)
QUAD = range(4)


def lanes(j):
    return slice(j * LANES, (j + 1) * LANES)


def octet(i):
    return pl.ds(8 * i, 8)


def remote(src, dst, ssem, rsem, rep, ep):
    return pltpu.make_async_remote_copy(src_ref=src, dst_ref=dst, send_sem=ssem, recv_sem=rsem,
                                        device_id={'replica': rep, 'ep': ep}, device_id_type=pl.DeviceIdType.MESH)


def meet(peers):
    barrier = pltpu.get_barrier_semaphore()
    for rep, ep in peers:
        pl.semaphore_signal(barrier, device_id={'replica': rep, 'ep': ep}, device_id_type=pl.DeviceIdType.MESH)
    pl.semaphore_wait(barrier, len(peers))


def place(nr, ne):
    side, nz = math.isqrt(nr), ne // 2
    r, e = lax.axis_index('replica'), lax.axis_index('ep')
    z, c = e // 2, e % 2
    px, py = r // side, r % side
    qx, qy = px % 2, py % 2
    nx, ny = 1 - qx, 1 - qy

    def quad(x, y):
        return (px - qx + x) * side + py - qy + y

    return types.SimpleNamespace(
        r=r, e=e, z=z, c=c, q=2 * qx + qy, par=(qx + qy) % 2, far=nz // 2, nz=nz, mate=e + 1 - 2 * c,
        beside=(quad(nx, qy), quad(qx, ny), quad(nx, ny)), seqs=(2 * nx + qy, 2 * qx + ny, 2 * nx + ny),
        ring=((e + 2) % ne, (e + ne - 2) % ne), quad=lambda j: quad(j // 2, j % 2),
        step=lambda way, dist: (z + (nz - dist if way else dist)) % nz)


def rmsnorm(v):
    v = v.astype(jnp.float32)
    return v * lax.rsqrt(jnp.mean(v * v, axis=-1, keepdims=True) + EPS)


ALONG = (1, 2, 3, 5, 6, 7)
BESIDE = (6, 7)


def attention_kernel(x_hbm, idx_hbm, wq_hbm, wk_hbm, wv_hbm, wo_hbm, cos_ref, sin_ref, h_ref, idx_ref, *rest, nr, ne, runs):
    u_refs = rest[:len(runs)]
    (xall, wqkv, stage, wov, obuf, orecv, acc, lsem, xs_s, xs_r, ix_s, ix_r, wd_s, wd_r, od_r, oo_r,
     wa_s, wa_r, wb_s, wb_r, oz_s, oz_r, oxy_s, oxy_r, od_s, oo_s) = rest[len(runs):]
    me = place(nr, ne)
    r, e, z, c, q, par, far, nz, mate, ring = me.r, me.e, me.z, me.c, me.q, me.par, me.far, me.nz, me.mate, me.ring
    events = 3 * far - 1
    s, d = x_hbm.shape
    wrows, cols = wqkv.shape[1] // ne, wqkv.shape[2]
    orows = wov.shape[1] // 2
    quart = s // 4
    unit = orows // 16
    mine = 2 * q + c

    def came(way, dist):
        return me.step(1 - way, dist)

    def al(v, m):
        return pl.multiple_of(v, m)

    loads = [pltpu.make_async_copy(x_hbm, xall.at[mine], lsem.at[0])]
    for w, ref in enumerate((wq_hbm, wk_hbm, wv_hbm)):
        loads.append(pltpu.make_async_copy(ref.at[:, pl.ds(al(mine * cols, cols), cols)],
                                           wqkv.at[w, pl.ds(al(e * wrows, wrows), wrows)], lsem.at[1 + w]))
        loads.append(pltpu.make_async_copy(ref.at[:, pl.ds(al((2 * q + 1 - c) * cols, cols), cols)],
                                           stage.at[w, z], lsem.at[4 + w]))
    loads.append(pltpu.make_async_copy(wo_hbm, wov.at[z, pl.ds(al(c * orows, orows), orows)], lsem.at[7]))
    loads.append(pltpu.make_async_copy(idx_hbm, idx_ref.at[q], lsem.at[8]))
    for cp in loads:
        cp.start()

    meet([(rep, ep) for rep in me.beside for ep in (e, mate)] + [(r, mate), (r, ring[0]), (r, ring[1])])
    for cp in loads:
        cp.wait()

    sent = []

    def go(make, *key):
        make(*key).start()
        sent.append((make, key))

    def part_a(zz):
        return wqkv.at[:, pl.ds(al((2 * zz + c) * wrows, wrows), wrows)]

    def part_b(zz):
        return stage.at[:, zz]

    def ring_a(way, dist, hop=1):
        at = part_a(came(way, dist - hop))
        return remote(at, at, wa_s.at[way, dist - 1], wa_r.at[way, dist - 1], r, ring[way])

    def ring_b(way, dist, hop=1):
        at = part_b(came(way, dist - hop))
        return remote(at, at, wb_s.at[way, dist - 1], wb_r.at[way, dist - 1], r, ring[way])

    def cross_w(way, dist):
        zz = came(way, dist)
        k = dist if way == 0 else nz - dist
        return remote(part_b(zz), part_a(zz), wd_s.at[k], wd_r.at[zz], r, mate)

    def x_to(k):
        at = xall.at[mine]
        return remote(at, at, xs_s.at[k], xs_r.at[mine], (*me.beside, r)[k], mate if k == len(me.beside) else e)

    def x_on(k):
        at = xall.at[2 * me.seqs[k] + c]
        return remote(at, at, xs_s.at[4 + k], xs_r.at[2 * me.seqs[k] + c], r, mate)

    def idx_to(k):
        return remote(idx_hbm, idx_ref.at[q], ix_s.at[k], ix_r.at[q], me.beside[k], e)

    def order(way, i):
        return (1 + i // 3, i % 3) if i < events - 2 else (far, way if i == events - 2 else 2)

    def rows_o(zz, dist, kind, p, way):
        if kind < 2:
            first, n = (16 - 2 * FU) * unit * p + FU * unit * kind, FU * unit
        elif dist < far:
            first, n = 2 * FU * unit, (16 - 4 * FU) * unit
        else:
            first, n = (2 * FU + (8 - 2 * FU) * way) * unit, (8 - 2 * FU) * unit
        return wov.at[zz, pl.ds(al(c * orows + first, unit), n)]

    def ring_o(way, i, hop=1):
        dist, kind = order(way, i)
        at = rows_o(came(way, dist - hop), dist, kind, par, way)
        return remote(at, at, oz_s.at[way, i], oz_r.at[way, i], r, ring[way])

    def side_o(way, i, p=par):
        dist, kind = order(way, i)
        at = rows_o(came(way, dist), dist, kind, p, way)
        return remote(at, at, oxy_s.at[way, i], oxy_r.at[way, i], me.beside[kind], e)

    def cross_o(way, i, other):
        dist, kind = order(way, i)
        zz = came(way, dist)
        at = rows_o(zz, dist, kind, 1 - par if other else par, way)
        return remote(at, at, od_s.at[2 * other + way, i], od_r.at[zz], r, mate)

    def own_o():
        at = wov.at[z, pl.ds(al(c * orows, orows), orows)]
        return remote(at, at, od_s.at[4, 0], od_r.at[z], r, mate)

    for way in WAYS:
        go(ring_a, way, 1)
    for way in WAYS:
        go(ring_b, way, 1)
    go(cross_w, 0, 0)
    for k in QUAD:
        go(x_to, k)
    for k in range(len(me.beside)):
        go(idx_to, k)

    def wait_w(dist):
        for way in WAYS:
            if dist <= far - way:
                ring_a(way, dist, 0).wait_recv()
                if dist + 1 <= far - way:
                    go(ring_a, way, dist + 1)
        for way in WAYS:
            if dist <= far - 1 + way:
                ring_b(way, dist, 0).wait_recv()
                if dist + 1 <= far - 1 + way:
                    go(ring_b, way, dist + 1)
                go(cross_w, way, dist)

    def pass_x(k):
        x_on(k).wait_recv()
        go(x_on, k)

    def serve(i):
        for way in WAYS:
            dist, kind = order(way, i)
            ring_o(way, i, 0).wait_recv()
            if dist + 1 < far:
                go(ring_o, way, i + 3)
            elif dist < far and kind in (way, 2):
                go(ring_o, way, events - 2 + (kind == 2))
            if kind < 2:
                go(side_o, way, i)
            go(cross_o, way, i, 0)

    def serve_side(i):
        for way in WAYS:
            side_o(way, i, 1 - par).wait_recv()
            go(cross_o, way, i, 1)

    for dist in range(1, far):
        wait_w(dist)
        if dist == max(1, far - 2):
            pass_x(0)
            pass_x(1)
    for i in range(3):
        for way in WAYS:
            go(ring_o, way, i)
    go(own_o)
    pass_x(2)
    wait_w(far)
    for zz in range(nz):
        at = wqkv.at[:, pl.ds((2 * zz + 1 - c) * wrows, wrows)]
        remote(at, at, wd_s.at[0], wd_r.at[zz], r, mate).wait_recv()
    for j in QUAD:
        at = xall.at[2 * j + 1 - c]
        remote(at, at, xs_s.at[0], xs_r.at[2 * j + 1 - c], r, mate).wait_recv()

    nh = cols // HEAD
    scale = 1.0 / math.sqrt(HEAD)

    def o_to(t, k):
        return remote(obuf.at[t, pl.ds(quart * k, quart)], orecv.at[mine, pl.ds(al(quart * (t // 2), quart), quart)],
                      oo_s.at[t, k], oo_r.at[mine], me.quad(k), 2 * z + t % 2)

    def send_o(t):
        for k in QUAD:
            @pl.when((q != k) | (c != t % 2))
            def _():
                o_to(t, k).start()

            @pl.when((q == k) & (c == t % 2))
            def _():
                orecv[mine, pl.ds(al(quart * (t // 2), quart), quart), :] = obuf[t, pl.ds(quart * k, quart), :]

    def sequence(t, carry):
        a = rmsnorm(xall[t]).astype(jnp.bfloat16)
        qf, kf, vf = [jnp.dot(a, wqkv[w], preferred_element_type=jnp.float32) for w in range(wqkv.shape[0])]
        cs, sn = cos_ref[...], sin_ref[...]
        row = lax.broadcasted_iota(jnp.int32, (s, s), 0)
        col = lax.broadcasted_iota(jnp.int32, (s, s), 1)
        for n in range(nh):
            at = slice(n * HEAD, (n + 1) * HEAD)
            qh, kh = qf[:, at], kf[:, at]
            qh = (qh * cs + pltpu.roll(qh, HEAD // 2, 1) * sn).astype(jnp.bfloat16)
            kh = (kh * cs + pltpu.roll(kh, HEAD // 2, 1) * sn).astype(jnp.bfloat16)
            sc = lax.dot_general(qh, kh, (((1,), (1,)), ((), ())), preferred_element_type=jnp.float32) * scale
            sc = jnp.where(row >= col, sc, -1e30)
            p = jnp.exp(sc - jnp.max(sc, axis=-1, keepdims=True))
            p = (p * (1.0 / jnp.sum(p, axis=-1, keepdims=True))).astype(jnp.bfloat16)
            obuf[t, :, at] = jnp.dot(p, vf[:, at].astype(jnp.bfloat16), preferred_element_type=jnp.float32).astype(jnp.bfloat16)

        @pl.when(t > 0)
        def _():
            send_o(t - 1)
        for i, n in enumerate(ALONG):
            @pl.when(t == n)
            def _():
                serve(i)
        for i, n in enumerate(BESIDE):
            @pl.when(t == n)
            def _():
                serve_side(i)
        return carry

    lax.fori_loop(0, nz, sequence, 0)
    send_o(nz - 1)
    serve_side(3)
    serve(6)
    serve_side(4)
    serve(7)

    for k in range(nz):
        @pl.when(k != mine)
        def _():
            at = orecv.at[k]
            remote(at, at, oo_s.at[0, 0], oo_r.at[k], r, mate).wait_recv()

    for j in QUAD:
        acc[pl.ds(quart * j, quart), :] = xall[2 * j + c, pl.ds(al(quart * q, quart), quart), :].astype(jnp.float32)

    def project(way, dist):
        zz = came(way, dist)
        at = wov.at[zz, pl.ds(al((1 - c) * orows, orows), orows)]
        remote(at, at, od_s.at[0, 0], od_r.at[zz], r, mate).wait_recv()
        width = min(512, d)

        def chunk(n, carry):
            cut = pl.ds(al(n * width, width), width)
            acc[:, cut] = acc[:, cut] + jnp.dot(orecv[zz], wov[zz, :, cut], preferred_element_type=jnp.float32)
            return carry

        lax.fori_loop(0, d // width, chunk, 0)

    def both(dist):
        for way in WAYS:
            project(way, dist)

    project(0, 0)
    both(1)
    serve(8)
    serve_side(6)
    serve_side(7)
    both(2)
    serve(9)
    serve(10)
    both(3)
    serve_side(9)
    project(0, far)
    h_ref[...] = acc[...].astype(jnp.bfloat16)
    acc[...] = rmsnorm(h_ref[...])
    first = 0
    for run, u_ref in zip(runs, u_refs):
        for j in QUAD:
            u_ref[run * j:run * (j + 1), :] = acc[quart * j + first:quart * j + first + run, :].astype(jnp.bfloat16)
        first += run
    for k in range(len(me.beside)):
        at = idx_ref.at[me.seqs[k]]
        remote(idx_hbm, at, ix_s.at[k], ix_r.at[me.seqs[k]], me.beside[k], e).wait_recv()
    for t in range(nz):
        for k in QUAD:
            @pl.when((q != k) | (c != t % 2))
            def _():
                o_to(t, k).wait_send()
    for make, key in sent:
        make(*key).wait_send()


def attention_call(x, idx, wq, wk, wv, wo, nr, ne, runs):
    s, d = x.shape
    nz = ne // 2
    events = 3 * (nz // 2) - 1
    half = HEAD // 2
    freq = THETA ** (-np.arange(half, dtype=np.float32) / half)
    ang = np.arange(s, dtype=np.float32)[:, None] * freq.astype(np.float32)
    cos, sin = np.cos(ang), np.sin(ang)
    cos = np.concatenate([cos, cos], axis=1)
    sin = np.concatenate([-sin, sin], axis=1)
    any_ = pl.BlockSpec(memory_space=pl.ANY)
    vmem = pl.BlockSpec(memory_space=pltpu.VMEM)
    bf = jnp.bfloat16
    dma = pltpu.SemaphoreType.DMA
    heads = pltpu.VMEM((nz, s, wq.shape[1] // nz), bf)
    h, ids, *us = pl.pallas_call(
        functools.partial(attention_kernel, nr=nr, ne=ne, runs=runs),
        out_shape=(jax.ShapeDtypeStruct((s, d), bf), jax.ShapeDtypeStruct((len(QUAD),) + idx.shape, idx.dtype),
                   *[jax.ShapeDtypeStruct((len(QUAD) * run, d), bf) for run in runs]),
        in_specs=[any_, any_, any_, any_, any_, any_, vmem, vmem],
        out_specs=(vmem, vmem, *[vmem for _ in runs]),
        scratch_shapes=[
            pltpu.VMEM((nz, s, d), bf),
            pltpu.VMEM((3, d, wq.shape[1] // nz), bf),
            pltpu.VMEM((3, nz, d // ne, wq.shape[1] // nz), bf),
            pltpu.VMEM((nz, 2 * wo.shape[0], d), bf),
            heads, heads,
            pltpu.VMEM((s, d), jnp.float32),
            dma((9,)), *[dma((nz,))] * 8, *[dma((2, events))] * 8, dma((5, events)), dma((nz, len(QUAD))),
        ],
        compiler_params=pltpu.CompilerParams(collective_id=0, has_side_effects=True, vmem_limit_bytes=60 * 2**20),
        cost_estimate=pl.CostEstimate(flops=100 * 10**9, bytes_accessed=30 * 10**6, transcendentals=10**6),
        name='attention',
    )(x, idx, wq, wk, wv, wo, jnp.asarray(cos), jnp.asarray(sin))
    return h, us, ids


def expert_kernel(nsp_ref, dense_ref, list_ref, glist_ref, gate_ref, u_hbm, w1, w3, w2, out_hbm,
                  uw, acc, ubuf, wup, wdown, act, xs, zs, up_sem, down_sem, in_sem, out_sem, *, cap, run):
    ne, d, f = w1.shape
    t = u_hbm.shape[0]
    ndev = t // (4 * run)
    per = ndev // 2
    blk = per * run
    nb = t // blk
    seg = d // LANES
    eight = 8 * seg
    wide = 4 * LANES

    def tile(g, j):
        return pl.ds(g * eight + 8 * j, 8)

    def fetch_up(slot, e):
        for k, w in enumerate((w1, w3)):
            pltpu.make_async_copy(w.at[e], wup.at[slot, k], up_sem.at[slot, k]).start()

    nd = wdown.shape[0]

    def fetch_down(e):
        e = jnp.asarray(e, jnp.int32)
        pltpu.make_async_copy(w2.at[e], wdown.at[e % nd], down_sem.at[e % nd]).start()

    def load(b):
        b = jnp.asarray(b, jnp.int32)
        j, first = b // (nb // 4), (b % (nb // 4)) * per
        for k in range(per):
            src = u_hbm.at[pl.ds(pl.multiple_of(((first + k) * 4 + j) * run, run), run)]
            pltpu.make_async_copy(src, ubuf.at[b % 2, pl.ds(k * run, run)], in_sem.at[b % 2]).start()

    load(0)
    load(1)
    fetch_up(0, 0)
    fetch_down(0)

    def clear(i, carry):
        acc[pl.ds(pl.multiple_of(i * eight, eight), eight), :] = jnp.zeros((eight, LANES), jnp.float32)
        return carry

    lax.fori_loop(0, t // 8 + 1, clear, 0)
    uw[pl.ds(t * seg, eight), :] = jnp.zeros((eight, LANES), jnp.float32)

    def widen(b, carry):
        at = ubuf.at[b % 2]
        pltpu.make_async_copy(at, at, in_sem.at[b % 2]).wait()
        to = uw.at[pl.ds(pl.multiple_of(b * blk * seg, eight), blk * seg)]
        for g in range(0, blk // 8, 2):
            for j in range(seg):
                for n, v in enumerate(jnp.split(at[8 * g:8 * g + 16, lanes(j)].astype(jnp.float32), 2)):
                    to[tile(g + n, j), :] = v

        @pl.when(b + 2 < nb)
        def _():
            load(b + 2)
        return carry

    lax.fori_loop(0, nb, widen, 0)
    x = ubuf.at[0]

    def narrow(src, rows):
        for g in range(0, rows // 8, 2):
            for j in range(seg):
                pair = [src[tile(g + n, j), :] for n in WAYS]
                x[8 * g:8 * g + 16, lanes(j)] = jnp.concatenate(pair).astype(jnp.bfloat16)

    def hidden(slot, rows):
        for c in range(0, f, 256):
            a1 = jnp.dot(x[:rows, :], wup[slot, 0, :, c:c + 256], preferred_element_type=jnp.float32)
            a3 = jnp.dot(x[:rows, :], wup[slot, 1, :, c:c + 256], preferred_element_type=jnp.float32)
            act[:rows, c:c + 256] = (jax.nn.silu(a1) * a3).astype(jnp.bfloat16)

    def expert(e, carry):
        slot = lax.rem(e, 2)

        @pl.when(e + 1 < ne)
        def _():
            fetch_up(1 - slot, e + 1)
            if nd == 2:
                fetch_down(e + 1)

        for j in WAYS:
            pltpu.make_async_copy(wup.at[slot, j], wup.at[slot, j], up_sem.at[slot, j]).wait()
        down = wdown.at[e % nd]
        pltpu.make_async_copy(down, down, down_sem.at[e % nd]).wait()

        def block(b, carry):
            @pl.when(dense_ref[e * nb + b] != 0)
            def _():
                part = pl.ds(pl.multiple_of(b * blk * seg, eight), blk * seg)
                narrow(uw.at[part], blk)
                hidden(slot, blk)
                g8 = gate_ref[b].T[:blk]
                lane = lax.broadcasted_iota(jnp.int32, g8.shape, 1)
                gate = jnp.sum(jnp.where(lane == e, g8, 0.0), axis=1, keepdims=True)
                to = acc.at[part]
                for c in range(0, d, wide):
                    z = jnp.dot(act[:blk, :], down[:, c:c + wide], preferred_element_type=jnp.float32)
                    z = z.astype(jnp.bfloat16).astype(jnp.float32)
                    z = jnp.where(gate != 0.0, gate * z, 0.0)
                    for g in range(blk // 8):
                        for j in range(wide // LANES):
                            at = tile(g, c // LANES + j)
                            to[at, :] = to[at, :] + z[8 * g:8 * g + 8, lanes(j)]
            return carry

        lax.fori_loop(0, nb, block, 0)
        n = nsp_ref[e]

        def gathered(i, carry):
            base = e * cap + i * SPM
            groups = (jnp.minimum(n - i * SPM, SPM) + 7) // 8

            def token(first):
                return pl.ds(first, seg, stride=8)

            def gather(q, carry):
                for s in range(8):
                    xs[token(q * eight + s), :] = uw[token(list_ref[base + q * 8 + s]), :]
                return carry

            lax.fori_loop(0, groups, gather, 0)
            narrow(xs, SPM)
            hidden(slot, SPM)
            for c in range(0, d, wide):
                z = jnp.dot(act[:SPM, :], down[:, c:c + wide], preferred_element_type=jnp.float32)
                z = z.astype(jnp.bfloat16).astype(jnp.float32)
                for g in range(SPM // 8):
                    for j in range(wide // LANES):
                        zs[tile(g, c // LANES + j), :] = z[8 * g:8 * g + 8, lanes(j)]

            def scatter(q, carry):
                for s in range(8):
                    i = base + q * 8 + s
                    at = token(list_ref[i])
                    acc[at, :] = acc[at, :] + glist_ref[i] * zs[token(q * eight + s), :]
                return carry

            lax.fori_loop(0, groups, scatter, 0)
            return carry

        lax.fori_loop(0, (n + SPM - 1) // SPM, gathered, 0)

        if nd == 1:
            @pl.when(e + 1 < ne)
            def _():
                fetch_down(e + 1)
        return carry

    lax.fori_loop(0, ne, expert, 0)

    def store(k, carry):
        for j in QUAD:
            src = acc.at[pl.ds(pl.multiple_of((j * ndev + k) * run * seg, run * seg), run * seg)]
            dst = out_hbm.at[pl.ds(pl.multiple_of((k * 4 + j) * run * seg, run * seg), run * seg)]
            pltpu.make_async_copy(src, dst, out_sem).start()
        return carry

    lax.fori_loop(0, ndev, store, 0)
    pltpu.make_async_copy(acc.at[pl.ds(0, t * seg)], out_hbm, out_sem).wait()


def expert_call(u, gates, nsp, dense, rows, glist, w1, w3, w2, run):
    t, d = u.shape
    ne, _, f = w1.shape
    cap = rows.shape[0] // ne
    seg = d // LANES
    blk = t // 8
    dma = pltpu.SemaphoreType.DMA

    def rows_of(n):
        return pltpu.VMEM((n * seg, LANES), jnp.float32)

    any_ = pl.BlockSpec(memory_space=pl.ANY)
    smem = pl.BlockSpec(memory_space=pltpu.SMEM)
    return pl.pallas_call(
        functools.partial(expert_kernel, cap=cap, run=run),
        out_shape=jax.ShapeDtypeStruct((t * seg, LANES), jnp.float32),
        in_specs=[smem] * 4 + [pl.BlockSpec(memory_space=pltpu.VMEM)] + [any_] * 4,
        out_specs=any_,
        scratch_shapes=[
            rows_of(t + 8), rows_of(t + 8),
            pltpu.VMEM((2, max(blk, SPM), d), jnp.bfloat16),
            pltpu.VMEM((2, 2, d, f), jnp.bfloat16),
            pltpu.VMEM((2 if t <= 2048 else 1, f, d), jnp.bfloat16),
            pltpu.VMEM((max(blk, SPM), f), jnp.bfloat16),
            rows_of(SPM), rows_of(SPM),
            dma((2, 2)), dma((2,)), dma((2,)), dma(()),
        ],
        compiler_params=pltpu.CompilerParams(vmem_limit_bytes=63 * 2**20),
        cost_estimate=pl.CostEstimate(flops=60 * 10**9, bytes_accessed=160 * 10**6, transcendentals=10**6),
        name='experts',
    )(nsp, dense, rows, glist, gates, u, w1, w3, w2)


def plan(ids, g, eids, d):
    t = ids.shape[0]
    ne = eids.shape[0]
    nb = 8
    blk = t // nb
    cap = nb * DENSE_AT
    seg = d // LANES
    eq = ids[:, :, None] == eids
    gates = jnp.sum(jnp.where(eq, g[:, :, None], 0.0), axis=1)
    m = jnp.any(eq, axis=1)
    dense = jnp.sum(m.reshape(nb, blk, ne), axis=1, dtype=jnp.int32) >= DENSE_AT
    sp = m & ~jnp.repeat(dense, blk, axis=0)
    spb = sp.astype(jnp.bfloat16).reshape(-1, LANES, ne)

    def ahead(n):
        i = jnp.arange(n)
        return (i < i[:, None]).astype(jnp.bfloat16)

    inner = jnp.einsum('ij,bje->bie', ahead(LANES), spb, preferred_element_type=jnp.float32)
    outer = jnp.einsum('ij,jke->ie', ahead(t // LANES), spb, preferred_element_type=jnp.float32)
    pos = jnp.where(sp, (inner + outer[:, None]).reshape(t, ne).astype(jnp.int32), -1)
    nsp = jnp.sum(sp, axis=0, dtype=jnp.int32)
    at = pos.T[:, None] == jnp.arange(cap)[:, None]
    tok = jnp.arange(t)
    start = (tok // 8) * (8 * seg) + tok % 8 - t * seg
    rows = jnp.sum(jnp.where(at, start, 0), axis=-1, dtype=jnp.int32) + t * seg
    glist = jnp.sum(jnp.where(at, gates.T[:, None], 0.0), axis=-1)
    gates = jnp.pad(gates.reshape(nb, blk, ne).transpose(0, 2, 1), ((0, 0), (0, 0), (0, -blk % LANES)))
    return gates, nsp, dense.T.reshape(-1).astype(jnp.int32), rows.reshape(-1), glist.reshape(-1)


def combine_kernel(acc_hbm, moe_ref, h_ref, y_ref, own, other, passed, ybuf, lsem, cs_s, cs_r, rs_s, rs_r, ys_s, ys_r,
                   *, nr, ne, runs):
    me = place(nr, ne)
    r, e, z, c, q, far, nz, mate, ring, to = me.r, me.e, me.z, me.c, me.q, me.far, me.nz, me.mate, me.ring, me.step
    quart = y_ref.shape[0] // 4
    seg = y_ref.shape[1] // LANES
    eight = 8 * seg
    rows = own.shape[1]
    half = rows // 2

    def block(ep):
        return acc_hbm.at[pl.ds(pl.multiple_of(ep * rows, rows), rows)]

    near = [(0, far)] + [(way, dist) for dist in range(far - 1, 0, -1) for way in WAYS] + [(0, 0)]

    def load(k):
        zz = to(*near[k])
        return pltpu.make_async_copy(block(2 * zz + c), own.at[zz], lsem.at[k])

    def cross(k):
        zz = to(*near[k])
        return remote(block(2 * zz + 1 - c), other.at[zz], cs_s.at[k], cs_r.at[k], r, mate)

    def cut(h):
        return pl.ds(h * half, half)

    def source(way, dist, h):
        first = dist == far or (dist == far - 1 and h != way)
        return own.at[to(way, dist), cut(h)] if first else passed.at[way, dist, cut(h)]

    def hop(way, dist, h):
        return remote(source(way, dist, h), passed.at[way, dist - 1, cut(h)], rs_s.at[way, dist, h], rs_r.at[way, dist - 1, h],
                      r, ring[way])

    def came(way, dist, h):
        at = passed.at[way, dist, cut(h)]
        return remote(at, at, rs_s.at[way, dist, h], rs_r.at[way, dist, h], r, ring[way])

    def y_to(n, j):
        return remote(ybuf.at[j, pl.ds(sum(runs[:n]), runs[n])], y_ref.at[pl.ds(pl.multiple_of(quart * q + sum(runs[:n]), 8), runs[n])],
                      ys_s.at[n, j], ys_r.at[n, q], me.quad(j), e)

    def y_from(n, j):
        at = y_ref.at[pl.ds(quart * j + sum(runs[:n]), runs[n])]
        return remote(at, at, ys_s.at[n, j], ys_r.at[n, j], me.beside[0], e)

    for k in range(nz):
        load(k).start()
    meet([(rep, e) for rep in me.beside] + [(r, mate), (r, ring[0]), (r, ring[1])])
    for k in range(nz):
        cross(k).start()

    def give(n, j):
        @pl.when(q != j)
        def _():
            y_to(n, j).start()

        @pl.when(q == j)
        def _():
            y_ref[pl.ds(pl.multiple_of(quart * q + sum(runs[:n]), 8), runs[n]), :] = ybuf[j, sum(runs[:n]):sum(runs[:n + 1]), :]

    def finish(n, j, moe):
        first = sum(runs[:n])
        for i in range(runs[n] // 8):
            part = moe(i)
            for m in range(seg):
                at = slice(m * LANES, (m + 1) * LANES)
                hf = h_ref[quart * j + first + 8 * i:quart * j + first + 8 * i + 8, at].astype(jnp.float32)
                ybuf[j, first + 8 * i:first + 8 * i + 8, at] = (hf + part[8 * m:8 * m + 8]).astype(jnp.bfloat16)

    done = 0
    for n in range(len(runs) - 1):
        for j in QUAD:
            at = done + runs[n] * j
            finish(n, j, lambda i, at=at: moe_ref[(at // 8 + i) * eight:(at // 8 + i + 1) * eight, :])
        for j in QUAD:
            give(n, j)
        done += 4 * runs[n]

    def ready(k):
        load(k).wait()
        cross(k).wait_recv()
        zz = to(*near[k])

        def add(i, carry):
            at = pl.ds(pl.multiple_of(i * eight, eight), eight)
            own[zz, at, :] = own[zz, at, :] + other[zz, at, :]
            return carry

        lax.fori_loop(0, rows // eight, add, 0)

    def join(way, dist, h):
        came(way, dist, h).wait_recv()
        zz = to(way, dist)

        def add(i, carry):
            at = pl.ds(pl.multiple_of(h * half + i * eight, eight), eight)
            passed[way, dist, at, :] = passed[way, dist, at, :] + own[zz, at, :]
            return carry

        lax.fori_loop(0, half // eight, add, 0)

    ready(0)
    for way in WAYS:
        hop(way, far, way).start()
    k = 1
    for dist in range(far - 1, 0, -1):
        for way in WAYS:
            ready(k)
            k += 1
            if dist == far - 1:
                hop(way, dist, 1 - way).start()
        for late in WAYS:
            for way in WAYS:
                h = way if late else 1 - way
                if dist == far - 1 and not late:
                    continue
                join(way, dist, h)
                hop(way, dist, h).start()
    ready(k)
    last = len(runs) - 1
    for h in WAYS:
        join(0, 0, h)
    for h in WAYS:
        came(1, 0, h).wait_recv()
    per = runs[last] // 8
    for j in QUAD:
        def moe(i, j=j):
            at = slice((j * per + i) * eight, (j * per + i + 1) * eight)
            return passed[0, 0, at, :] + passed[1, 0, at, :]

        finish(last, j, moe)
    for j in QUAD:
        give(last, j)
    for n in range(len(runs)):
        for j in QUAD:
            @pl.when(q != j)
            def _():
                y_from(n, j).wait_recv()
                y_to(n, j).wait_send()
    for k in range(nz):
        cross(k).wait_send()
    for way in WAYS:
        hop(way, far, way).wait_send()
        for dist in range(1, far):
            for h in WAYS:
                hop(way, dist, h).wait_send()


def combine_call(acc, moe, h, nr, ne, runs):
    s, d = h.shape
    nz = ne // 2
    rows = acc.shape[0] // ne
    dma = pltpu.SemaphoreType.DMA
    vmem = pl.BlockSpec(memory_space=pltpu.VMEM)
    sums = pltpu.VMEM((nz, rows, LANES), jnp.float32)
    hops, back = dma((2, nz, 2)), dma((len(runs), len(QUAD)))
    return pl.pallas_call(
        functools.partial(combine_kernel, nr=nr, ne=ne, runs=runs),
        out_shape=jax.ShapeDtypeStruct((s, d), jnp.bfloat16),
        in_specs=[pl.BlockSpec(memory_space=pl.ANY), vmem, vmem],
        out_specs=vmem,
        scratch_shapes=[
            sums, sums, pltpu.VMEM((2, nz // 2, rows, LANES), jnp.float32),
            pltpu.VMEM((len(QUAD), sum(runs), d), jnp.bfloat16),
            *[dma((nz,))] * 3, hops, hops, back, back,
        ],
        compiler_params=pltpu.CompilerParams(collective_id=1, has_side_effects=True, vmem_limit_bytes=48 * 2**20),
        cost_estimate=pl.CostEstimate(flops=100 * 10**9, bytes_accessed=30 * 10**6, transcendentals=10**6),
        name='combine',
    )(acc, moe, h)


def router(h, wr, ids):
    r = rmsnorm(h)
    logits = jnp.dot(r, wr, precision=lax.Precision.HIGHEST, preferred_element_type=jnp.float32)
    hot = ids[:, :, None] == jnp.arange(wr.shape[1], dtype=jnp.int32)
    picked = jnp.sum(jnp.where(hot, logits[:, None, :], 0.0), axis=-1)
    return jax.nn.softmax(picked, axis=-1)


def solution(mesh):
    nr, nd = mesh.shape['replica'], mesh.shape['ep']
    side = math.isqrt(nr)
    tok, split = P(('replica', 'ep')), P('ep')

    def local(x, wq, wk, wv, wo, wr, w1, w3, w2, idx):
        b, s, d = x.shape
        t, k, ne = b * s, idx.shape[-1], w1.shape[0]
        me = lax.axis_index('ep')
        rep = lax.axis_index('replica')
        quart = t // 4
        runs = tuple(n * quart // 64 for n in RUNS)
        h, us, ids = attention_call(x.reshape(t, d), idx.reshape(t, k).T, wq, wk, wv, wo, nr, nd, runs)
        us = [lax.all_gather(u, 'ep', axis=0, tiled=True) for u in us]
        mine = 2 * (rep // side % 2) + rep % side % 2
        ids = lax.dynamic_slice_in_dim(ids.transpose(0, 2, 1), mine * quart, quart, axis=1).reshape(t, k)
        g = router(h, wr, ids)
        gi = lax.all_gather(jnp.concatenate([g, ids.astype(jnp.float32)], axis=1), 'ep', axis=0, tiled=False)
        gi = gi.reshape(nd, 4, quart, 2 * k)
        eids = me * ne + jnp.arange(ne)
        first = 0
        for u, run in zip(us, runs):
            part = gi[:, :, first:first + run].transpose(1, 0, 2, 3).reshape(-1, 2 * k)
            acc = expert_call(u, *plan(part[:, k:].astype(jnp.int32), part[:, :k], eids, d), w1, w3, w2, run)
            first += run
            if first < quart:
                moe = lax.psum_scatter(acc, 'ep', scatter_dimension=0, tiled=True)
        return combine_call(acc, moe, h, nr, nd, runs).reshape(b, s, d)

    return jax.shard_map(local, mesh=mesh,
                         in_specs=(tok, split, split, split, split, P(), split, split, split, tok),
                         out_specs=tok, check_vma=False)
```
